32 devices in a mesh: row: 8 (over y, x, core), col: 4 (over z).
Axes of the slice: x: 2, y: 2, z: 4, core: 2. Of those that a mesh axis runs over, the one named last changes fastest.
Arguments:
- object_field: float32 [2, 3072, 1536], P(None, 'row', 'col'), may hold values from -4 to 4
- illumination: float32 [2, 256, 256], replicated, may hold values from -4 to 4
- measured: float32 [8, 4, 8, 256, 256], P('row', 'col'), may hold values from 0.05 to 4
- positions: int32 [8, 4, 8, 2], P('row', 'col'), may hold values from 0 to 383
- frame_counts: int32 [8, 4], P('row', 'col'), may hold values from 1 to 8, as said below
- first_count: int32 [8, 4], P('row', 'col'), may hold values from 0 to 4
Outputs:
- new_object: float32 [2, 3072, 1536], P(None, 'row', 'col')
- new_illumination: float32 [2, 256, 256], replicated
The draws below stay inside these ranges and needn't reach their ends.
Inputs may be any that keep to these rules, and one draw needn't show every extreme that they name: `frame_counts`: some tile has exactly 8 live frames in every draw; slots from a tile's count on are unused.
All inputs are finite; a program needn't handle non-finite values.
Results may differ from the reference program's by a relative error of at most 0.0003.
Values sent between devices are 32-bit elements; how exact they have to be, the bound alone decides.
No kernel may reach another device: no remote copies, remote signals or barrier semaphores. Data moves between devices by JAX's collectives and lax.ppermute only.
A program may use at most 64 MiB of HBM per device.

```python
import math
import jax
import jax.numpy as jnp
from jax import lax

TILE = 384
PROBE = 256
FRAMES = 8
TR = 8
TC = 4
NX = 3072
NY = 1536


def draw_frame_counts(key, part):
    key_drawn = jax.random.fold_in(key, 101)
    key_heavy = jax.random.fold_in(key, 202)
    key_chosen = jax.random.fold_in(key, 303)
    lowest = max(1, FRAMES // 4)
    highest = max(lowest, FRAMES // 2)
    drawn = jax.random.randint(key_drawn, (TR, TC), lowest, highest + 1)
    is_heavy = jax.random.randint(key_heavy, (TR, TC), 0, 8) == 0
    chosen = jax.random.randint(key_chosen, (), 0, TR * TC)
    flat_index = jnp.arange(TR * TC, dtype=jnp.int32).reshape(TR, TC)
    return jnp.where(is_heavy | (flat_index == chosen), FRAMES, drawn).astype(jnp.int32)


def touch_ends(result, own_key, smallest, largest):
    longest = result.shape.index(max(result.shape))
    spots = []
    for shift in (0, 1):
        where = [jax.random.randint(jax.random.fold_in(own_key, axis), (), 0, length) for axis, length in enumerate(result.shape)]
        where[longest] = (where[longest] + shift) % result.shape[longest]
        spots.append(tuple(where))
    return result.at[spots[0]].set(smallest).at[spots[1]].set(largest)


def block_levels(stream_key, extent, cuts, smallest, largest):
    def one(axis_at, blocks):
        steps = jax.random.uniform(jax.random.fold_in(jax.random.fold_in(stream_key, 6), axis_at), (blocks,), jnp.float32, smallest / len(cuts), largest / len(cuts))
        return jnp.repeat(jnp.exp(steps), extent[axis_at] // blocks).reshape((-1,) + (1,) * (len(extent) - axis_at - 1))

    level = one(*cuts[0])
    for cut in cuts[1:]:
        level = level * one(*cut)
    return level


def noise(stream_key, extent, scale, reach, split=(), kind=jnp.bfloat16):
    entries = scale * jax.random.normal(stream_key, extent, jnp.float32)
    if split:
        entries = entries * block_levels(stream_key, extent, split, -0.22, 0.18)
    return jnp.clip(entries, -reach, reach).astype(kind)


def setup_inputs(seed: int = 0) -> dict:
    streams_of = jax.random.split(jax.random.key(seed), 7)
    return {
        "object_field": noise(streams_of[0], (2, NX, NY), 0.7, 4.0, ((1, 8), (2, 4)), jnp.float32),
        "illumination": noise(streams_of[1], (2, PROBE, PROBE), 0.7, 4.0, (), jnp.float32),
        "measured": jnp.clip(jnp.exp(math.log(4.0) - 4.3820266 * jax.random.uniform(streams_of[2], (TR, TC, FRAMES, PROBE, PROBE), jnp.float32) ** block_levels(streams_of[2], (TR, TC, FRAMES, PROBE, PROBE), ((0, 8), (1, 4)), -0.2, 0.2)), 0.05, 4.0),
        "positions": touch_ends(jax.random.randint(streams_of[3], (TR, TC, FRAMES, 2), 0, TILE), jax.random.fold_in(streams_of[3], 1), 0, TILE - 1).astype(jnp.int32),
        "frame_counts": draw_frame_counts(jax.random.fold_in(streams_of[6], 71), 0),
        "first_count": touch_ends(jax.random.randint(streams_of[5], (TR, TC), 0, FRAMES // 2 + 1), jax.random.fold_in(streams_of[5], 1), 0, (FRAMES // 2 + 1) - 1).astype(jnp.int32),
    }


def dft_tables(length):
    index_row = jnp.arange(length, dtype=jnp.int32)
    product = index_row[:, None] * index_row[None, :] % length
    angle = product.astype(jnp.float32) * (2.0 * math.pi / length)
    scale = 1.0 / math.sqrt(length)
    return (jnp.cos(angle) * scale, -jnp.sin(angle) * scale)

def matmul(left, right):
    return jnp.dot(left, right, precision=lax.Precision.HIGHEST)

def complex_product(left_real, left_imag, right_real, right_imag):
    return (matmul(left_real, right_real) - matmul(left_imag, right_imag), matmul(left_real, right_imag) + matmul(left_imag, right_real))

def frame_gradients(object_patch, illumination, intensity, tables):
    table_real, table_imag = tables
    patch_real, patch_imag = (object_patch[0], object_patch[1])
    probe_real, probe_imag = (illumination[0], illumination[1])
    exit_real = probe_real * patch_real - probe_imag * patch_imag
    exit_imag = probe_real * patch_imag + probe_imag * patch_real
    half_real, half_imag = complex_product(table_real, table_imag, exit_real, exit_imag)
    wave_real, wave_imag = complex_product(half_real, half_imag, table_real, table_imag)
    residue = wave_real * wave_real + wave_imag * wave_imag - intensity
    back_real, back_imag = complex_product(table_real, -table_imag, residue * wave_real, residue * wave_imag)
    grad_real, grad_imag = complex_product(back_real, back_imag, table_real, -table_imag)
    object_term = jnp.stack([probe_real * grad_real + probe_imag * grad_imag, probe_real * grad_imag - probe_imag * grad_real])
    probe_term = jnp.stack([patch_real * grad_real + patch_imag * grad_imag, patch_real * grad_imag - patch_imag * grad_real])
    return (object_term, probe_term)

def reference(object_field, illumination, measured, positions, frame_counts, first_count):
    tables = dft_tables(PROBE)
    step_size = 0.5 / math.sqrt(TR * TC * FRAMES)
    anchor = jnp.zeros((), jnp.int32)
    for batch_index in range(2):
        padded = jnp.pad(object_field, ((0, 0), (0, PROBE), (0, PROBE)))

        def add_frame(slot_index, running):
            slot_index = jnp.asarray(slot_index).astype(jnp.int32)
            tile_row = slot_index // (TC * FRAMES)
            tile_col = slot_index // FRAMES % TC
            frame_slot = slot_index % FRAMES
            live_frames = frame_counts[tile_row, tile_col]
            first_frames = jnp.minimum(first_count[tile_row, tile_col], live_frames)
            if batch_index == 0:
                is_live = frame_slot < first_frames
            else:
                is_live = (frame_slot >= first_frames) & (frame_slot < live_frames)

            def accumulate(state):
                grad_object, grad_probe = state
                row_start = (tile_row * TILE + positions[tile_row, tile_col, frame_slot, 0]).astype(jnp.int32)
                col_start = (tile_col * TILE + positions[tile_row, tile_col, frame_slot, 1]).astype(jnp.int32)
                object_patch = lax.dynamic_slice(padded, (anchor, row_start, col_start), (2, PROBE, PROBE))
                intensity = measured[tile_row, tile_col, frame_slot]
                object_term, probe_term = frame_gradients(object_patch, illumination, intensity, tables)
                current = lax.dynamic_slice(grad_object, (anchor, row_start, col_start), (2, PROBE, PROBE))
                grad_object = lax.dynamic_update_slice(grad_object, current + object_term, (anchor, row_start, col_start))
                return (grad_object, grad_probe + probe_term)

            def unchanged(state):
                return state
            return lax.cond(is_live, accumulate, unchanged, running)
        start_state = (jnp.zeros_like(padded), jnp.zeros_like(illumination))
        grad_object, grad_probe = lax.fori_loop(0, TR * TC * FRAMES, add_frame, start_state)
        object_field = object_field - 0.1 * grad_object[:, :NX, :NY]
        illumination = illumination - step_size * grad_probe
    return (object_field, illumination)
```

```python
import math

import jax
import jax.numpy as jnp
import numpy as np
from jax import lax
from jax.experimental import pallas as pl
from jax.experimental.pallas import tpu as pltpu
from jax.sharding import PartitionSpec as P

LANES = 128


def shift(value, axis, steps):
    count = lax.axis_size(axis)
    leading, last = (max(0, -steps), min(count, count - steps))
    return lax.ppermute(value, axis, [(source, source + steps) for source in range(leading, last)])


def split(value):
    high = value.astype(jnp.bfloat16)
    low = (value - high.astype(jnp.float32)).astype(jnp.bfloat16)
    return high, low


def half_tables(length):
    half = length // 2
    m = np.arange(half)[:, None]
    n = np.arange(half)[None, :]
    tables = []
    for odd in (0, 1):
        angle = ((2 * m + odd) * n % length) * (2.0 * math.pi / length)
        c, s = np.cos(angle) / math.sqrt(length), np.sin(angle) / math.sqrt(length)
        real = np.block([[c, s], [-s, c]])
        tables += [real, real.T]
    stacked = np.stack(tables)
    high = stacked.astype(jnp.bfloat16)
    low = (stacked - high.astype(np.float64)).astype(jnp.bfloat16)
    return jnp.asarray(np.concatenate([high, low]))


def sorter(length):
    half = length // 2
    rows = np.arange(length)
    source = np.where(rows < half, 2 * rows, 2 * (rows - half) + 1)
    return jnp.asarray(np.eye(length)[source].astype(jnp.bfloat16))


def dot(left, right):
    return jnp.dot(left, right, preferred_element_type=jnp.float32)


def sort_kernel(sorter_ref, unsorter_ref, in_ref, out_ref):
    def three(value):
        high, mid = split(value)
        low = (value - high.astype(jnp.float32) - mid.astype(jnp.float32)).astype(jnp.bfloat16)
        return high, mid, low

    high, mid, low = three(in_ref[0])
    columns = dot(high, unsorter_ref[...]) + dot(mid, unsorter_ref[...]) + dot(low, unsorter_ref[...])
    high, mid, low = three(columns)
    out_ref[0] = dot(sorter_ref[...], high) + dot(sorter_ref[...], mid) + dot(sorter_ref[...], low)


def sort_measured(measured):
    slots, length, _ = measured.shape
    order = sorter(length)
    whole = pl.BlockSpec((length, length), lambda s: (0, 0))
    frame = pl.BlockSpec((1, length, length), lambda s: (s, 0, 0))
    return pl.pallas_call(
        sort_kernel,
        grid=(slots,),
        in_specs=[whole, whole, frame],
        out_specs=frame,
        out_shape=jax.ShapeDtypeStruct(measured.shape, jnp.float32),
        name="sort_measured",
    )(order, order.T, measured)


def frame_loop(start, stop, pos_ref, tab_ref, probe_ref, sorted_ref, ext, grad, gprobe_ref, win, pro):
    length = probe_ref.shape[1]
    half = length // 2
    me, met, mo, mot, le, let, lo, lot = (tab_ref.at[i] for i in range(8))

    def left(high_table, low_table, high, low):
        return dot(high_table[...], high) + dot(high_table[...], low) + dot(low_table[...], high)

    def right(high, low, high_table, low_table):
        return dot(high, high_table[...]) + dot(low, high_table[...]) + dot(high, low_table[...])

    def frame(slot, carry):
        row = pos_ref[slot, 0]
        col = pos_ref[slot, 1]
        tile = lax.shift_right_logical(col, 7)
        turn = lax.bitwise_and(col, LANES - 1)
        lane = lax.broadcasted_iota(jnp.int32, (length, LANES), 1)
        first = lane >= turn
        rows = pl.ds(row, length)
        for p in range(2):
            a, b = pltpu.roll(probe_ref[p, :, :LANES], turn, 1), pltpu.roll(probe_ref[p, :, LANES:], turn, 1)
            pro[p, :, :LANES] = jnp.where(first, a, b)
            pro[p, :, LANES:] = jnp.where(first, b, a)
            win[p, :, :LANES] = jnp.where(first, ext[p, tile, rows, :], ext[p, tile + 2, rows, :])
            win[p, :, LANES:] = ext[p, tile + 1, rows, :]

        def leave(at):
            pr, pi, wr, wi = (pro[0, at, :], pro[1, at, :], win[0, at, :], win[1, at, :])
            return pr * wr - pi * wi, pr * wi + pi * wr

        tr, ti = leave(pl.ds(0, half))
        br, bi = leave(pl.ds(half, half))
        uh, ul = split(jnp.concatenate([tr + br, ti + bi], axis=0))
        vh, vl = split(jnp.concatenate([tr - br, ti - bi], axis=0))
        even = left(me, le, uh, ul)
        odd = left(mo, lo, vh, vl)

        def fold(block):
            r, i = block[:half], block[half:]
            ra, rb, ia, ib = (r[:, :LANES], r[:, LANES:], i[:, :LANES], i[:, LANES:])
            return (
                jnp.concatenate([ra + rb, ia + ib], axis=1),
                jnp.concatenate([ra - rb, ia - ib], axis=1),
            )

        eu, ev = fold(even)
        ou, ov = fold(odd)
        uh, ul = split(jnp.concatenate([eu, ou], axis=0))
        vh, vl = split(jnp.concatenate([ev, ov], axis=0))
        wave_even = right(uh, ul, met, let)
        wave_odd = right(vh, vl, mot, lot)

        def weigh(wave, target):
            r, i = wave[:, :LANES], wave[:, LANES:]
            residue = r * r + i * i - target
            return split(jnp.concatenate([residue * r, residue * i], axis=1))

        eh, el = weigh(wave_even, sorted_ref[slot, :, :LANES])
        oh, ol = weigh(wave_odd, sorted_ref[slot, :, LANES:])
        e = right(eh, el, me, le)
        o = right(oh, ol, mo, lo)
        near, far = e + o, e - o

        def rejoin(at):
            return split(
                jnp.concatenate(
                    [
                        jnp.concatenate([near[at, :LANES], far[at, :LANES]], axis=1),
                        jnp.concatenate([near[at, LANES:], far[at, LANES:]], axis=1),
                    ],
                    axis=0,
                )
            )

        eh, el = rejoin(slice(0, half))
        oh, ol = rejoin(slice(half, length))
        e = left(met, let, eh, el)
        o = left(mot, lot, oh, ol)
        for back, at in ((e + o, 0), (e - o, half)):
            gr, gi = back[:half], back[half:]
            chunk = pl.ds(at, half)
            pr, pi = pro[0, chunk, :], pro[1, chunk, :]
            wr, wi = win[0, chunk, :], win[1, chunk, :]
            here = pl.ds(row + at, half)
            mask = first[:half]
            for p, term in ((0, pr * gr + pi * gi), (1, pr * gi - pi * gr)):
                side, mid = term[:, :LANES], term[:, LANES:]
                grad[p, tile, here, :] = grad[p, tile, here, :] + jnp.where(mask, side, 0.0)
                grad[p, tile + 1, here, :] = grad[p, tile + 1, here, :] + mid
                grad[p, tile + 2, here, :] = grad[p, tile + 2, here, :] + jnp.where(mask, 0.0, side)
            unturn = lax.bitwise_and(LANES - turn, LANES - 1)
            keep = lane[:half] < LANES - turn
            for p, term in ((0, wr * gr + wi * gi), (1, wr * gi - wi * gr)):
                a, b = pltpu.roll(term[:, :LANES], unturn, 1), pltpu.roll(term[:, LANES:], unturn, 1)
                gprobe_ref[p, chunk, :LANES] = gprobe_ref[p, chunk, :LANES] + jnp.where(keep, a, b)
                gprobe_ref[p, chunk, LANES:] = gprobe_ref[p, chunk, LANES:] + jnp.where(keep, b, a)
        return carry

    lax.fori_loop(start, stop, frame, 0)


def batch_kernel(batch, cuts, *refs):
    count_ref, first_ref, pos_ref, tab_ref, probe_ref, sorted_ref = refs[:6]
    pieces = refs[6 : 6 + len(cuts[0])]
    outs = refs[6 + len(cuts[0]) : -5]
    send_ref, keep_ref, outs = outs[-2], outs[-1], outs[:-2]
    ext, grad, win, pro, gprobe_ref = refs[-5:]
    core = lax.bitwise_and(lax.axis_index("row"), 1)
    for piece, (r, c) in zip(pieces, cuts[0]):
        for p in range(2):
            for j in range(piece.shape[2] // LANES):
                ext[p, c // LANES + j, r : r + piece.shape[1], :] = piece[p, :, j * LANES : (j + 1) * LANES]
    grad[...] = jnp.zeros_like(grad)
    gprobe_ref[...] = jnp.zeros_like(gprobe_ref)
    live = count_ref[0, 0]
    edge = jnp.minimum(first_ref[0, 0], live)
    start, stop = (0, edge) if batch == 0 else (edge, live)
    frame_loop(start, stop, pos_ref, tab_ref, probe_ref, sorted_ref, ext, grad, gprobe_ref, win, pro)
    send_ref[...] = gprobe_ref[1 - core]
    keep_ref[...] = gprobe_ref[core]
    for out, (r, c) in zip(outs, cuts[1]):
        for p in range(2):
            for j in range(out.shape[2] // LANES):
                out[p, :, j * LANES : (j + 1) * LANES] = grad[p, c // LANES + j, r : r + out.shape[1], :]


def run_batch(batch, scalars, tables, probe, sorted_measured, pieces, places, wanted):
    length = probe.shape[1]
    side = max(r + piece.shape[1] for piece, (r, c) in zip(pieces, places))
    cols = max(c + piece.shape[2] for piece, (r, c) in zip(pieces, places))
    smem = pl.BlockSpec(memory_space=pltpu.SMEM)
    vmem = pl.BlockSpec(memory_space=pltpu.VMEM)
    out_shape = [jax.ShapeDtypeStruct((2, rows, width), jnp.float32) for r, c, rows, width in wanted]
    out_shape += [jax.ShapeDtypeStruct(probe.shape[1:], jnp.float32)] * 2
    cuts = (tuple(places), tuple((r, c) for r, c, _, _ in wanted))
    tiles = cols // LANES
    return pl.pallas_call(
        lambda *refs: batch_kernel(batch, cuts, *refs),
        in_specs=[smem, smem, smem] + [vmem] * (3 + len(pieces)),
        out_specs=[vmem] * len(out_shape),
        out_shape=out_shape,
        scratch_shapes=[
            pltpu.VMEM((2, tiles, side, LANES), jnp.float32),
            pltpu.VMEM((2, tiles, side, LANES), jnp.float32),
            pltpu.VMEM(probe.shape, jnp.float32),
            pltpu.VMEM(probe.shape, jnp.float32),
            pltpu.VMEM(probe.shape, jnp.float32),
        ],
        compiler_params=pltpu.CompilerParams(vmem_limit_bytes=56 * 1024 * 1024),
        name=f"batch_{batch}",
    )(*scalars, tables, probe, sorted_measured, *pieces)


def swap(value, axis, mask):
    count = lax.axis_size(axis)
    return lax.ppermute(value, axis, [(source, source ^ mask) for source in range(count)])


def vmem_call(kernel, out_shape, name, *operands):
    return pl.pallas_call(
        kernel,
        in_specs=[pl.BlockSpec(memory_space=pltpu.VMEM)] * len(operands),
        out_specs=jax.tree.map(lambda _: pl.BlockSpec(memory_space=pltpu.VMEM), out_shape),
        out_shape=out_shape,
        name=name,
    )(*operands)


def row_bits():
    row = lax.axis_index("row")
    return lax.bitwise_and(row, 1), lax.shift_right_logical(row, 1)


def deal_kernel(keep_ref, heard_ref, *outs):
    _, seat = row_bits()
    height = outs[0].shape[0]
    for j, out in enumerate(outs):
        rows = pl.ds(pl.multiple_of(lax.bitwise_xor(seat, j) * height, height), height)
        out[...] = keep_ref[rows, :] + heard_ref[rows, :]


def sum_probe(send, keep):
    members = lax.axis_size("row") // 2
    height, width = keep.shape[0] // members, keep.shape[1]
    piece = jax.ShapeDtypeStruct((height, width), jnp.float32)
    dealt = vmem_call(deal_kernel, [piece] * members, "deal", keep, swap(send, "row", 1))
    total = dealt[0]
    for value in [swap(dealt[j], "row", 2 * j) for j in range(1, members)]:
        total = total + value
    step = 1
    while step < lax.axis_size("col"):
        near = swap(total, "col", step)
        if 2 * step < lax.axis_size("col"):
            far, farther = swap(total, "col", 2 * step), swap(total, "col", 3 * step)
            total = (total + near) + (far + farther)
        else:
            total = total + near
        step *= 4
    plane = jnp.concatenate([total] + [swap(total, "row", 2 * j) for j in range(1, members)], axis=0)
    return plane, swap(plane, "row", 1)


def step_probe(old_ref, plane_ref, other_ref, new_ref, step_size):
    core, seat = row_bits()
    members = lax.axis_size("row") // 2
    height = plane_ref.shape[0] // members
    for j in range(members):
        rows = pl.ds(pl.multiple_of(lax.bitwise_xor(seat, j) * height, height), height)
        here = slice(j * height, (j + 1) * height)
        new_ref[core, rows, :] = old_ref[core, rows, :] - step_size * plane_ref[here, :]
        new_ref[1 - core, rows, :] = old_ref[1 - core, rows, :] - step_size * other_ref[here, :]


def finish_kernel(nl_ref, nm_ref, ll_ref, lm_ref, own_ref, up_ref, lt_ref, low_ref, out_ref):
    n = nl_ref.shape[1]
    top, low, lft, mid = slice(0, n), slice(n, None), slice(0, n), slice(n, None)
    for p in range(2):
        out_ref[p, top, lft] = nl_ref[p] - 0.1 * (own_ref[p, top, lft] + up_ref[p, :, lft] + lt_ref[p])
        out_ref[p, top, mid] = nm_ref[p] - 0.1 * (own_ref[p, top, mid] + up_ref[p, :, mid])
        out_ref[p, low, lft] = ll_ref[p] - 0.1 * (own_ref[p, low, lft] + low_ref[p])
        out_ref[p, low, mid] = lm_ref[p] - 0.1 * own_ref[p, low, mid]


def per_device(object_field, illumination, measured, positions, frame_counts, first_count):
    n = illumination.shape[1]
    tile = object_field.shape[1]
    k = tile - n
    devices = lax.axis_size("row") * lax.axis_size("col")
    step_size = 0.5 / math.sqrt(devices * measured.shape[2])
    tables = half_tables(n)
    scalars = (frame_counts, first_count, positions[0, 0])
    sorted_measured = sort_measured(measured[0, 0])
    o = object_field

    right_top = shift(o[:, :n, :n], "col", -1)
    below = shift(o[:, :n, :], "row", -1)
    right_low = shift(o[:, n:, :n], "col", -1)
    corner = shift(right_top, "row", -1)
    places = [(0, 0), (0, tile), (n, tile), (tile, 0), (tile, tile)]
    pieces = [o, right_top, right_low, below, corner]
    wanted = [(tile, 0, n, n), (tile, n, n, k), (tile, tile, n, n), (0, 0, tile, tile), (0, tile, n, n), (n, tile, k, n)]
    down_l, down_m, down_r, own, rt, rl, send, keep = run_batch(
        0, scalars, tables, illumination, sorted_measured, pieces, places, wanted
    )
    from_up_r = shift(down_r, "row", 1)
    from_up_l = shift(down_l, "row", 1)
    from_left_low = shift(rl, "col", 1)
    from_right_low = shift(own[:, n:, :n], "col", -1)
    from_up_m = shift(down_m, "row", 1)
    send_r = rt + from_up_r
    from_left_top = shift(send_r, "col", 1)
    send_l = own[:, :n, :n] + from_up_l
    from_right_top = shift(send_l, "col", -1)
    inside = (lax.axis_index("col") < lax.axis_size("col") - 1).astype(jnp.float32)
    new_m = o[:, :n, n:] - 0.1 * (own[:, :n, n:] + from_up_m)
    new_l = o[:, :n, :n] - 0.1 * (send_l + from_left_top)
    new_r = right_top - (0.1 * inside) * (send_r + from_right_top)
    below_m = shift(new_m, "row", -1)
    below_l = shift(new_l, "row", -1)
    below_r = shift(new_r, "row", -1)
    low_l = o[:, n:, :n] - 0.1 * (own[:, n:, :n] + from_left_low)
    low_m = o[:, n:, n:] - 0.1 * own[:, n:, n:]
    low_r = right_low - (0.1 * inside) * (rl + from_right_low)
    step_kernel = lambda *refs: step_probe(*refs, step_size)
    probe_shape = jax.ShapeDtypeStruct(illumination.shape, jnp.float32)
    probe = vmem_call(step_kernel, probe_shape, "step_probe", illumination, *sum_probe(send, keep))

    pieces = [new_l, new_m, new_r, low_l, low_m, low_r, below_l, below_m, below_r]
    places = [(r, c) for r in (0, n, tile) for c in (0, n, tile)]
    wanted = [(tile, 0, n, tile), (tile, tile, n, n), (0, 0, tile, tile), (0, tile, n, n), (n, tile, k, n)]
    down, down_r, own, rt, rl, send, keep = run_batch(
        1, scalars, tables, probe, sorted_measured, pieces, places, wanted
    )
    from_up_r = shift(down_r, "row", 1)
    from_left_low = shift(rl, "col", 1)
    from_up = shift(down, "row", 1)
    from_left_top = shift(rt + from_up_r, "col", 1)
    new_object = vmem_call(
        finish_kernel,
        jax.ShapeDtypeStruct(o.shape, jnp.float32),
        "finish",
        new_l, new_m, low_l, low_m, own, from_up, from_left_top, from_left_low,
    )
    new_probe = vmem_call(step_kernel, probe_shape, "step_probe", probe, *sum_probe(send, keep))
    return (new_object, new_probe)


def solution(mesh):
    in_specs = (
        P(None, "row", "col"),
        P(),
        P("row", "col", None, None, None),
        P("row", "col", None, None),
        P("row", "col"),
        P("row", "col"),
    )
    out_specs = (P(None, "row", "col"), P())
    return jax.shard_map(
        per_device, mesh=mesh, in_specs=in_specs, out_specs=out_specs, check_vma=False
    )
```

```python
import math

import jax
import jax.numpy as jnp
import numpy as np
from jax import lax
from jax.experimental import pallas as pl
from jax.experimental.pallas import tpu as pltpu
from jax.sharding import PartitionSpec as P


LANES = 128


def shift(value, axis, steps):
    count = lax.axis_size(axis)
    leading, last = (max(0, -steps), min(count, count - steps))
    return lax.ppermute(value, axis, [(source, source + steps) for source in range(leading, last)])


def split(value):
    high = value.astype(jnp.bfloat16)
    low = (value - high.astype(jnp.float32)).astype(jnp.bfloat16)
    return high, low


def half_tables(length):
    half = length // 2
    m = np.arange(half)[:, None]
    n = np.arange(half)[None, :]
    tables = []
    for odd in (0, 1):
        angle = ((2 * m + odd) * n % length) * (2.0 * math.pi / length)
        c, s = np.cos(angle) / math.sqrt(length), np.sin(angle) / math.sqrt(length)
        real = np.block([[c, s], [-s, c]])
        tables += [real, real.T]
    stacked = np.stack(tables)
    high = stacked.astype(jnp.bfloat16)
    low = (stacked - high.astype(np.float64)).astype(jnp.bfloat16)
    return jnp.asarray(np.concatenate([high, low]))


def sorter(length):
    half = length // 2
    rows = np.arange(length)
    source = np.where(rows < half, 2 * rows, 2 * (rows - half) + 1)
    return jnp.asarray(np.eye(length)[source].astype(jnp.bfloat16))


def dot(left, right):
    return jnp.dot(left, right, preferred_element_type=jnp.float32)


def sort_kernel(count_ref, sorter_ref, unsorter_ref, in_ref, out_ref):
    def three(value):
        high, mid = split(value)
        low = (value - high.astype(jnp.float32) - mid.astype(jnp.float32)).astype(jnp.bfloat16)
        return high, mid, low

    def frame(slot, carry):
        high, mid, low = three(in_ref[slot])
        columns = dot(high, unsorter_ref[...]) + dot(mid, unsorter_ref[...]) + dot(low, unsorter_ref[...])
        high, mid, low = three(columns)
        out_ref[slot] = dot(sorter_ref[...], high) + dot(sorter_ref[...], mid) + dot(sorter_ref[...], low)
        return carry

    lax.fori_loop(0, count_ref[0, 0], frame, 0)


def frame_loop(start, stop, pos_ref, tab_ref, probe_ref, sorted_ref, ext, grad, gprobe_ref, win, pro):
    length = probe_ref.shape[1]
    half = length // 2
    me, met, mo, mot, le, let, lo, lot = (tab_ref.at[i] for i in range(8))

    def left(high_table, low_table, high, low):
        return dot(high_table[...], high) + dot(high_table[...], low) + dot(low_table[...], high)

    def right(high, low, high_table, low_table):
        return dot(high, high_table[...]) + dot(low, high_table[...]) + dot(high, low_table[...])

    def pair(step, carry):
        first_slot = start + 2 * step
        second_slot = jnp.minimum(first_slot + 1, stop - 1)
        slots = (first_slot, second_slot)
        alive = jnp.where(first_slot + 1 < stop, 1.0, 0.0)
        both = (0, 1)
        lane = lax.broadcasted_iota(jnp.int32, (length, LANES), 1)
        row = [pos_ref[s, 0] for s in slots]
        tile = [lax.shift_right_logical(pos_ref[s, 1], 7) for s in slots]
        turn = [lax.bitwise_and(pos_ref[s, 1], LANES - 1) for s in slots]

        def enter(f):
            first = lane >= turn[f]
            rows = pl.ds(row[f], length)
            for p in range(2):
                a = pltpu.roll(probe_ref[p, :, :LANES], turn[f], 1)
                b = pltpu.roll(probe_ref[p, :, LANES:], turn[f], 1)
                pro[f, p, :, :LANES] = jnp.where(first, a, b)
                pro[f, p, :, LANES:] = jnp.where(first, b, a)
                win[f, p, :, :LANES] = jnp.where(first, ext[p, tile[f], rows, :], ext[p, tile[f] + 2, rows, :])
                win[f, p, :, LANES:] = ext[p, tile[f] + 1, rows, :]

            def leave(at):
                pr, pi, wr, wi = (pro[f, 0, at, :], pro[f, 1, at, :], win[f, 0, at, :], win[f, 1, at, :])
                return pr * wr - pi * wi, pr * wi + pi * wr

            tr, ti = leave(pl.ds(0, half))
            br, bi = leave(pl.ds(half, half))
            uh, ul = split(jnp.concatenate([tr + br, ti + bi], axis=0))
            vh, vl = split(jnp.concatenate([tr - br, ti - bi], axis=0))
            return uh, ul, vh, vl

        def fold(block):
            r, i = block[:half], block[half:]
            ra, rb, ia, ib = (r[:, :LANES], r[:, LANES:], i[:, :LANES], i[:, LANES:])
            return (
                jnp.concatenate([ra + rb, ia + ib], axis=1),
                jnp.concatenate([ra - rb, ia - ib], axis=1),
            )

        def weigh(wave, target, f):
            r, i = wave[:, :LANES], wave[:, LANES:]
            residue = r * r + i * i - target
            if f:
                residue = residue * alive
            return split(jnp.concatenate([residue * r, residue * i], axis=1))

        def middle(even, odd, f):
            eu, ev = fold(even)
            ou, ov = fold(odd)
            uh, ul = split(jnp.concatenate([eu, ou], axis=0))
            vh, vl = split(jnp.concatenate([ev, ov], axis=0))
            wave_even = right(uh, ul, met, let)
            wave_odd = right(vh, vl, mot, lot)
            eh, el = weigh(wave_even, sorted_ref[slots[f], :, :LANES], f)
            oh, ol = weigh(wave_odd, sorted_ref[slots[f], :, LANES:], f)
            e = right(eh, el, me, le)
            o = right(oh, ol, mo, lo)
            near, far = e + o, e - o

            def rejoin(at):
                return split(
                    jnp.concatenate(
                        [
                            jnp.concatenate([near[at, :LANES], far[at, :LANES]], axis=1),
                            jnp.concatenate([near[at, LANES:], far[at, LANES:]], axis=1),
                        ],
                        axis=0,
                    )
                )

            return rejoin(slice(0, half)) + rejoin(slice(half, length))

        def exit_terms(f, e, o):
            mask = lane[:half] >= turn[f]
            unturn = lax.bitwise_and(LANES - turn[f], LANES - 1)
            keep = lane[:half] < LANES - turn[f]
            for back, at in ((e + o, 0), (e - o, half)):
                gr, gi = back[:half], back[half:]
                chunk = pl.ds(at, half)
                pr, pi = pro[f, 0, chunk, :], pro[f, 1, chunk, :]
                wr, wi = win[f, 0, chunk, :], win[f, 1, chunk, :]
                here = pl.ds(row[f] + at, half)
                for p, term in ((0, wr * gr + wi * gi), (1, wr * gi - wi * gr)):
                    a, b = pltpu.roll(term[:, :LANES], unturn, 1), pltpu.roll(term[:, LANES:], unturn, 1)
                    gprobe_ref[p, chunk, :LANES] = gprobe_ref[p, chunk, :LANES] + jnp.where(keep, a, b)
                    gprobe_ref[p, chunk, LANES:] = gprobe_ref[p, chunk, LANES:] + jnp.where(keep, b, a)
                for p, term in ((0, pr * gr + pi * gi), (1, pr * gi - pi * gr)):
                    side, mid = term[:, :LANES], term[:, LANES:]
                    grad[p, tile[f], here, :] = grad[p, tile[f], here, :] + jnp.where(mask, side, 0.0)
                    grad[p, tile[f] + 1, here, :] = grad[p, tile[f] + 1, here, :] + mid
                    grad[p, tile[f] + 2, here, :] = grad[p, tile[f] + 2, here, :] + jnp.where(mask, 0.0, side)

        entered = [enter(f) for f in both]
        halves = [(left(me, le, uh, ul), left(mo, lo, vh, vl)) for uh, ul, vh, vl in entered]
        joined = [middle(even, odd, f) for f, (even, odd) in zip(both, halves)]
        ends = [(left(met, let, eh, el), left(mot, lot, oh, ol)) for eh, el, oh, ol in joined]
        for f, (e, o) in zip(both, ends):
            exit_terms(f, e, o)
        return carry

    lax.fori_loop(0, lax.shift_right_logical(stop - start + 1, 1), pair, 0)


def seat_order(value_ref, core, seat, members, out_ref):
    height = out_ref.shape[0] // members
    for j in range(members):
        rows = pl.ds(pl.multiple_of(lax.bitwise_xor(seat, j) * height, height), height)
        out_ref[j * height : (j + 1) * height, :] = value_ref[core, rows, :]


def put(ext, piece, row, col):
    for p in range(2):
        for j in range(piece.shape[2] // LANES):
            ext[p, col // LANES + j, row : row + piece.shape[1], :] = piece[p, :, j * LANES : (j + 1) * LANES]


def first_kernel(*refs):
    count_ref, first_ref, pos_ref, tab_ref, probe_ref, sorted_ref = refs[:6]
    own, right_top, right_low, below, corner = refs[6:11]
    ext, grad, down0, up0, right1, left1, send_ref, keep_ref = refs[11:19]
    win, pro, gprobe_ref = refs[19:]
    n = probe_ref.shape[1]
    tile = own.shape[1]
    put(ext, own, 0, 0)
    put(ext, right_top, 0, tile)
    put(ext, right_low, n, tile)
    put(ext, below, tile, 0)
    put(ext, corner, tile, tile)
    grad[...] = jnp.zeros_like(grad)
    gprobe_ref[...] = jnp.zeros_like(gprobe_ref)
    stop = jnp.minimum(first_ref[0, 0], count_ref[0, 0])
    frame_loop(0, stop, pos_ref, tab_ref, probe_ref, sorted_ref, ext, grad, gprobe_ref, win, pro)
    core, seat = row_bits()
    members = lax.axis_size("row") // 2
    seat_order(gprobe_ref, 1 - core, seat, members, send_ref)
    seat_order(gprobe_ref, core, seat, members, keep_ref)
    t = tile // LANES
    down0[...] = grad[0, :, tile:, :]
    up0[...] = grad[0, :, :n, :]
    right1[...] = grad[1, t:, :, :]
    left1[...] = grad[1, : n // LANES, :, :]


def columns_kernel(grad, above, below, right0, left0):
    n, side = above.shape[1], grad.shape[2]
    t, w = grad.shape[1] - n // LANES, n // LANES
    for out, at in ((right0, slice(t, t + w)), (left0, slice(0, w))):
        out[:, :n, :] = grad[0, at, :n, :] + above[at]
        out[:, n : side - n, :] = grad[0, at, n : side - n, :]
        out[:, side - n :, :] = grad[0, at, side - n :, :] + below[at]


def rows_kernel(grad, before, after, down1, up1):
    w = before.shape[0]
    tiles, side = grad.shape[1], grad.shape[2]
    n = down1.shape[1]
    for out, at in ((down1, slice(side - n, side)), (up1, slice(0, n))):
        out[:w] = grad[1, :w, at, :] + before[:, at, :]
        out[w : tiles - w] = grad[1, w : tiles - w, at, :]
        out[tiles - w :] = grad[1, tiles - w :, at, :] + after[:, at, :]


def second_kernel(step_size, *refs):
    count_ref, first_ref, pos_ref, tab_ref, probe_ref, sorted_ref = refs[:6]
    old, g1, above0, below0, before0, after0, before1, after1, above1, below1, plane, other = refs[6:18]
    grad, new_ref, new_probe, down_r, down_l, low_r, send_ref, keep_ref = refs[18:26]
    ext, win, pro, gprobe_ref = refs[26:]
    n, side, tiles = probe_ref.shape[1], ext.shape[2], ext.shape[1]
    tile, w = side - n, n // LANES
    t = tile // LANES
    step_probe(probe_ref, plane, other, new_probe, step_size)
    inside_col = jnp.where(lax.axis_index("col") < lax.axis_size("col") - 1, 0.1, 0.0)
    inside_row = jnp.where(lax.axis_index("row") < lax.axis_size("row") - 1, 1.0, 0.0)
    for p, (above, below, before, after) in enumerate(
        ((above0, below0, before0, after0), (above1, below1, before1, after1))
    ):
        for j in range(tiles):
            weight = 0.1 if j < t else inside_col
            for r0, r1, side_rows in ((0, n, above), (n, tile, None), (tile, side, below)):
                total = g1[p, j, r0:r1, :]
                if side_rows is not None:
                    total = total + side_rows[j]
                if j < w:
                    total = total + before[j, r0:r1, :]
                if j >= t:
                    total = total + after[j - t, r0:r1, :]
                scale = weight * inside_row if r0 == tile else weight
                ext[p, j, r0:r1, :] = old[p, j, r0:r1, :] - scale * total
    for p in range(2):
        for j in range(t):
            new_ref[p, :, j * LANES : (j + 1) * LANES] = ext[p, j, :tile, :]
    grad[...] = jnp.zeros_like(grad)
    gprobe_ref[...] = jnp.zeros_like(gprobe_ref)
    stop = count_ref[0, 0]
    start = jnp.minimum(first_ref[0, 0], stop)
    frame_loop(start, stop, pos_ref, tab_ref, new_probe, sorted_ref, ext, grad, gprobe_ref, win, pro)
    core, seat = row_bits()
    members = lax.axis_size("row") // 2
    seat_order(gprobe_ref, 1 - core, seat, members, send_ref)
    seat_order(gprobe_ref, core, seat, members, keep_ref)
    down_r[...] = grad[:, t:, tile:, :]
    down_l[...] = grad[:, :t, tile:, :]
    low_r[...] = grad[:, t:, n:tile, :]


def join_kernel(grad, above, out):
    t, n = grad.shape[1] - above.shape[1], above.shape[2]
    out[...] = grad[:, t:, :n, :] + above[...]


def f32(*shape):
    return jax.ShapeDtypeStruct(shape, jnp.float32)


def vmem_call(kernel, out_shape, operands, scalars=(), scratch=(), limit=16):
    smem = [pl.BlockSpec(memory_space=pltpu.SMEM)] * len(scalars)
    vmem = pl.BlockSpec(memory_space=pltpu.VMEM)
    return pl.pallas_call(
        kernel,
        in_specs=smem + [vmem] * len(operands),
        out_specs=jax.tree.map(lambda _: vmem, out_shape),
        out_shape=out_shape,
        scratch_shapes=list(scratch),
        compiler_params=pltpu.CompilerParams(vmem_limit_bytes=limit * 1024 * 1024),
    )(*scalars, *operands)


def swap(value, axis, mask):
    count = lax.axis_size(axis)
    return lax.ppermute(value, axis, [(source, source ^ mask) for source in range(count)])


def row_bits():
    row = lax.axis_index("row")
    return lax.bitwise_and(row, 1), lax.shift_right_logical(row, 1)


def deal_kernel(keep_ref, heard_ref, *outs):
    height = outs[0].shape[0]
    for j, out in enumerate(outs):
        rows = slice(j * height, (j + 1) * height)
        out[...] = keep_ref[rows, :] + heard_ref[rows, :]


def steps_of(cols):
    steps = []
    step = 1
    while step < cols:
        steps.append(step)
        step *= 4
    return steps


def sum_probe(send, keep):
    members = lax.axis_size("row") // 2
    cols = lax.axis_size("col")
    height, width = keep.shape[0] // members, keep.shape[1]
    heard = swap(send, "row", 1)
    dealt = vmem_call(deal_kernel, [f32(height, width)] * members, (keep, heard))
    total = dealt[0]
    for value in [swap(dealt[j], "row", 2 * j) for j in range(1, members)]:
        total = total + value
    for step in steps_of(cols):
        near, *rest = [swap(total, "col", m * step) for m in (1, 2, 3) if m * step < cols]
        total = total + near
        if rest:
            total = total + (rest[0] + rest[1])
    parts = [total] + [swap(total, "row", 2 * j) for j in range(1, members)]
    plane = jnp.concatenate(parts, axis=0)
    return plane, swap(plane, "row", 1)


def step_probe(old_ref, plane_ref, other_ref, new_ref, step_size):
    core, seat = row_bits()
    members = lax.axis_size("row") // 2
    height = plane_ref.shape[0] // members
    for j in range(members):
        rows = pl.ds(pl.multiple_of(lax.bitwise_xor(seat, j) * height, height), height)
        here = slice(j * height, (j + 1) * height)
        new_ref[core, rows, :] = old_ref[core, rows, :] - step_size * plane_ref[here, :]
        new_ref[1 - core, rows, :] = old_ref[1 - core, rows, :] - step_size * other_ref[here, :]


def finish_kernel(old_ref, grad, above, before_top, before_low, out_ref):
    n, w = above.shape[2], before_top.shape[1]
    tile = out_ref.shape[1]
    for p in range(2):
        for j in range(tile // LANES):
            here = slice(j * LANES, (j + 1) * LANES)
            top = grad[p, j, :n, :] + above[p, j]
            low = grad[p, j, n:tile, :]
            if j < w:
                top = top + before_top[p, j]
                low = low + before_low[p, j]
            out_ref[p, :n, here] = old_ref[p, :n, here] - 0.1 * top
            out_ref[p, n:, here] = old_ref[p, n:, here] - 0.1 * low


def per_device(object_field, illumination, measured, positions, frame_counts, first_count):
    n = illumination.shape[1]
    tile = object_field.shape[1]
    side = tile + n
    tiles, w, t = side // LANES, n // LANES, tile // LANES
    devices = lax.axis_size("row") * lax.axis_size("col")
    step_size = 0.5 / math.sqrt(devices * measured.shape[2])
    tables = half_tables(n)
    scalars = (frame_counts, first_count, positions[0, 0])
    o = object_field

    right_top = shift(o[:, :n, :n], "col", -1)
    right_low = shift(o[:, n:, :n], "col", -1)
    below = shift(o[:, :n, :], "row", -1)
    order = sorter(n)
    sorted_measured = vmem_call(
        sort_kernel, f32(*measured.shape[2:]), (order, order.T, measured[0, 0]), (frame_counts,)
    )
    right_top, sorted_measured = lax.optimization_barrier((right_top, sorted_measured))
    corner = shift(right_top, "row", -1)

    work = [pltpu.VMEM((2,) + illumination.shape, jnp.float32)] * 2 + [pltpu.VMEM(illumination.shape, jnp.float32)]
    whole, plane_shape = f32(2, tiles, side, LANES), f32(n, n)
    row_strip, col_strip = f32(tiles, n, LANES), f32(w, side, LANES)
    ext, grad, down0, up0, right1, left1, send, keep = vmem_call(
        first_kernel,
        [whole, whole, row_strip, row_strip, col_strip, col_strip, plane_shape, plane_shape],
        (tables, illumination, sorted_measured, o, right_top, right_low, below, corner),
        scalars,
        work,
        28,
    )
    before1 = shift(right1, "col", 1)
    after1 = shift(left1, "col", -1)
    above0 = shift(down0, "row", 1)
    below0 = shift(up0, "row", -1)
    right0, left0 = vmem_call(columns_kernel, [col_strip] * 2, (grad, above0, below0))
    before0 = shift(right0, "col", 1)
    after0 = shift(left0, "col", -1)
    down1, up1 = vmem_call(rows_kernel, [row_strip] * 2, (grad, before1, after1))
    above1 = shift(down1, "row", 1)
    below1 = shift(up1, "row", -1)
    plane, other = sum_probe(send, keep)

    grad, new_object, new_probe, down_r, down_l, low_r, send, keep = vmem_call(
        lambda *refs: second_kernel(step_size, *refs),
        [whole, f32(*o.shape), f32(*illumination.shape), f32(2, w, n, LANES), f32(2, t, n, LANES),
         f32(2, w, tile - n, LANES), plane_shape, plane_shape],
        (tables, illumination, sorted_measured, ext, grad, above0, below0, before0, after0,
         before1, after1, above1, below1, plane, other),
        scalars,
        [pltpu.VMEM(whole.shape, jnp.float32)] + work,
        28,
    )
    above_r = shift(down_r, "row", 1)
    before_low = shift(low_r, "col", 1)
    above_l = shift(down_l, "row", 1)
    joined = vmem_call(join_kernel, f32(*above_r.shape), (grad, above_r))
    before_top = shift(joined, "col", 1)
    new_object = vmem_call(finish_kernel, f32(*o.shape), (new_object, grad, above_l, before_top, before_low))
    plane, other = sum_probe(send, keep)
    new_probe = vmem_call(
        lambda *refs: step_probe(*refs, step_size), f32(*illumination.shape), (new_probe, plane, other)
    )
    return (new_object, new_probe)


def solution(mesh):
    in_specs = (
        P(None, "row", "col"),
        P(),
        P("row", "col", None, None, None),
        P("row", "col", None, None),
        P("row", "col"),
        P("row", "col"),
    )
    out_specs = (P(None, "row", "col"), P())
    return jax.shard_map(per_device, mesh=mesh, in_specs=in_specs, out_specs=out_specs, check_vma=False)
```

```python
import math

import jax
import jax.numpy as jnp
import numpy as np
from jax import lax
from jax.experimental import pallas as pl
from jax.experimental.pallas import tpu as pltpu
from jax.sharding import PartitionSpec as P


LANES = 128


def shift(value, axis, steps):
    count = lax.axis_size(axis)
    leading, last = (max(0, -steps), min(count, count - steps))
    return lax.ppermute(value, axis, [(source, source + steps) for source in range(leading, last)])


def split(value):
    high = value.astype(jnp.bfloat16)
    low = (value - high.astype(jnp.float32)).astype(jnp.bfloat16)
    return high, low


def half_tables(length):
    half = length // 2
    m = np.arange(half)[:, None]
    n = np.arange(half)[None, :]
    tables = []
    for odd in (0, 1):
        angle = ((2 * m + odd) * n % length) * (2.0 * math.pi / length)
        c, s = np.cos(angle) / math.sqrt(length), np.sin(angle) / math.sqrt(length)
        real = np.block([[c, s], [-s, c]])
        tables += [real, real.T]
    stacked = np.stack(tables)
    high = stacked.astype(jnp.bfloat16)
    low = (stacked - high.astype(np.float64)).astype(jnp.bfloat16)
    return jnp.asarray(np.concatenate([high, low]))


def sorter(length):
    half = length // 2
    rows = np.arange(length)
    source = np.where(rows < half, 2 * rows, 2 * (rows - half) + 1)
    return jnp.asarray(np.eye(length)[source].astype(jnp.bfloat16))


def dot(left, right):
    return jnp.dot(left, right, preferred_element_type=jnp.float32)


def sort_kernel(count_ref, sorter_ref, unsorter_ref, in_ref, out_ref):
    def three(value):
        high, mid = split(value)
        low = (value - high.astype(jnp.float32) - mid.astype(jnp.float32)).astype(jnp.bfloat16)
        return high, mid, low

    def frame(slot, carry):
        high, mid, low = three(in_ref[slot])
        columns = dot(high, unsorter_ref[...]) + dot(mid, unsorter_ref[...]) + dot(low, unsorter_ref[...])
        high, mid, low = three(columns)
        out_ref[slot] = dot(sorter_ref[...], high) + dot(sorter_ref[...], mid) + dot(sorter_ref[...], low)
        return carry

    lax.fori_loop(0, count_ref[0, 0], frame, 0)


def frame_loop(start, stop, pos_ref, tab_ref, probe_ref, sorted_ref, ext, grad, gprobe_ref, win, pro):
    length = probe_ref.shape[1]
    half = length // 2
    me, met, mo, mot, le, let, lo, lot = (tab_ref.at[i] for i in range(8))

    def left(high_table, low_table, high, low):
        both_tables = dot(jnp.concatenate([high_table[...], low_table[...]], axis=0), high)
        return both_tables[:length] + both_tables[length:] + dot(high_table[...], low)

    def pair(step, carry):
        first_slot = start + 2 * step
        second_slot = jnp.minimum(first_slot + 1, stop - 1)
        slots = (first_slot, second_slot)
        alive = jnp.where(first_slot + 1 < stop, 1.0, 0.0)
        both = (0, 1)
        lane = lax.broadcasted_iota(jnp.int32, (length, LANES), 1)
        row = [pos_ref[s, 0] for s in slots]
        tile = [lax.shift_right_logical(pos_ref[s, 1], 7) for s in slots]
        turn = [lax.bitwise_and(pos_ref[s, 1], LANES - 1) for s in slots]

        def enter(f):
            first = lane >= turn[f]
            rows = pl.ds(row[f], length)
            for p in range(2):
                a = pltpu.roll(probe_ref[p, :, :LANES], turn[f], 1)
                b = pltpu.roll(probe_ref[p, :, LANES:], turn[f], 1)
                pro[f, p, :, :LANES] = jnp.where(first, a, b)
                pro[f, p, :, LANES:] = jnp.where(first, b, a)
                win[f, p, :, :LANES] = jnp.where(first, ext[p, tile[f], rows, :], ext[p, tile[f] + 2, rows, :])
                win[f, p, :, LANES:] = ext[p, tile[f] + 1, rows, :]

            def leave(at):
                pr, pi, wr, wi = (pro[f, 0, at, :], pro[f, 1, at, :], win[f, 0, at, :], win[f, 1, at, :])
                return pr * wr - pi * wi, pr * wi + pi * wr

            tr, ti = leave(pl.ds(0, half))
            br, bi = leave(pl.ds(half, half))
            uh, ul = split(jnp.concatenate([tr + br, ti + bi], axis=0))
            vh, vl = split(jnp.concatenate([tr - br, ti - bi], axis=0))
            return uh, ul, vh, vl

        def fold(block):
            r, i = block[:half], block[half:]
            ra, rb, ia, ib = (r[:, :LANES], r[:, LANES:], i[:, :LANES], i[:, LANES:])
            return (
                jnp.concatenate([ra + rb, ia + ib], axis=1),
                jnp.concatenate([ra - rb, ia - ib], axis=1),
            )

        def weigh(wave, target, f):
            r, i = wave[:, :LANES], wave[:, LANES:]
            residue = r * r + i * i - target
            if f:
                residue = residue * alive
            return split(jnp.concatenate([residue * r, residue * i], axis=1))

        def stacked(pairs, high_table, low_table):
            highs = [pair[0] for pair in pairs]
            size = length * len(highs)
            big = dot(jnp.concatenate(highs + [pair[1] for pair in pairs], axis=0), high_table[...])
            small = dot(jnp.concatenate(highs, axis=0), low_table[...])
            total = big[:size] + big[size:] + small
            return [total[f * length : (f + 1) * length] for f in both]

        def middle(halves):
            us, vs = [], []
            for even, odd in halves:
                eu, ev = fold(even)
                ou, ov = fold(odd)
                us.append(split(jnp.concatenate([eu, ou], axis=0)))
                vs.append(split(jnp.concatenate([ev, ov], axis=0)))
            wave_even = stacked(us, met, let)
            wave_odd = stacked(vs, mot, lot)
            es = [weigh(wave_even[f], sorted_ref[slots[f], :, :LANES], f) for f in both]
            os = [weigh(wave_odd[f], sorted_ref[slots[f], :, LANES:], f) for f in both]
            back_even = stacked(es, me, le)
            back_odd = stacked(os, mo, lo)
            results = []
            for e, o in zip(back_even, back_odd):
                near, far = e + o, e - o
                pieces = ()
                for at in (slice(0, half), slice(half, length)):
                    top = jnp.concatenate([near[at, :LANES], far[at, :LANES]], axis=1)
                    low = jnp.concatenate([near[at, LANES:], far[at, LANES:]], axis=1)
                    pieces += split(jnp.concatenate([top, low], axis=0))
                results.append(pieces)
            return results

        def exit_terms(f, e, o):
            mask = lane[:half] >= turn[f]
            unturn = lax.bitwise_and(LANES - turn[f], LANES - 1)
            keep = lane[:half] < LANES - turn[f]
            for back, at in ((e + o, 0), (e - o, half)):
                gr, gi = back[:half], back[half:]
                chunk = pl.ds(at, half)
                pr, pi = pro[f, 0, chunk, :], pro[f, 1, chunk, :]
                wr, wi = win[f, 0, chunk, :], win[f, 1, chunk, :]
                here = pl.ds(row[f] + at, half)
                for p, term in ((0, wr * gr + wi * gi), (1, wr * gi - wi * gr)):
                    a, b = pltpu.roll(term[:, :LANES], unturn, 1), pltpu.roll(term[:, LANES:], unturn, 1)
                    gprobe_ref[p, chunk, :LANES] = gprobe_ref[p, chunk, :LANES] + jnp.where(keep, a, b)
                    gprobe_ref[p, chunk, LANES:] = gprobe_ref[p, chunk, LANES:] + jnp.where(keep, b, a)
                for p, term in ((0, pr * gr + pi * gi), (1, pr * gi - pi * gr)):
                    side, mid = term[:, :LANES], term[:, LANES:]
                    grad[p, tile[f], here, :] = grad[p, tile[f], here, :] + jnp.where(mask, side, 0.0)
                    grad[p, tile[f] + 1, here, :] = grad[p, tile[f] + 1, here, :] + mid
                    grad[p, tile[f] + 2, here, :] = grad[p, tile[f] + 2, here, :] + jnp.where(mask, 0.0, side)

        entered = [enter(f) for f in both]
        halves = [(left(me, le, uh, ul), left(mo, lo, vh, vl)) for uh, ul, vh, vl in entered]
        joined = middle(halves)
        ends = [(left(met, let, eh, el), left(mot, lot, oh, ol)) for eh, el, oh, ol in joined]
        for f, (e, o) in zip(both, ends):
            exit_terms(f, e, o)
        return carry

    lax.fori_loop(0, lax.shift_right_logical(stop - start + 1, 1), pair, 0)


def seat_order(value_ref, core, seat, members, out_ref):
    height = out_ref.shape[0] // members
    for j in range(members):
        rows = pl.ds(pl.multiple_of(lax.bitwise_xor(seat, j) * height, height), height)
        out_ref[j * height : (j + 1) * height, :] = value_ref[core, rows, :]


def put(ext, piece, row, col):
    for p in range(2):
        for j in range(piece.shape[2] // LANES):
            ext[p, col // LANES + j, row : row + piece.shape[1], :] = piece[p, :, j * LANES : (j + 1) * LANES]


def first_kernel(*refs):
    count_ref, first_ref, pos_ref, tab_ref, probe_ref, sorted_ref = refs[:6]
    own, right_top, right_low, below, corner = refs[6:11]
    ext, grad, down0, up0, right1, left1, send_ref, keep_ref = refs[11:19]
    win, pro, gprobe_ref = refs[19:]
    n = probe_ref.shape[1]
    tile = own.shape[1]
    put(ext, own, 0, 0)
    put(ext, right_top, 0, tile)
    put(ext, right_low, n, tile)
    put(ext, below, tile, 0)
    put(ext, corner, tile, tile)
    grad[...] = jnp.zeros_like(grad)
    gprobe_ref[...] = jnp.zeros_like(gprobe_ref)
    stop = jnp.minimum(first_ref[0, 0], count_ref[0, 0])
    frame_loop(0, stop, pos_ref, tab_ref, probe_ref, sorted_ref, ext, grad, gprobe_ref, win, pro)
    core, seat = row_bits()
    members = lax.axis_size("row") // 2
    seat_order(gprobe_ref, 1 - core, seat, members, send_ref)
    seat_order(gprobe_ref, core, seat, members, keep_ref)
    t = tile // LANES
    down0[...] = grad[0, :, tile:, :]
    up0[...] = grad[0, :, :n, :]
    right1[...] = grad[1, t:, :, :]
    left1[...] = grad[1, : n // LANES, :, :]


def columns_kernel(grad, above, below, right0, left0):
    n, side = above.shape[1], grad.shape[2]
    t, w = grad.shape[1] - n // LANES, n // LANES
    for out, at in ((right0, slice(t, t + w)), (left0, slice(0, w))):
        out[:, :n, :] = grad[0, at, :n, :] + above[at]
        out[:, n : side - n, :] = grad[0, at, n : side - n, :]
        out[:, side - n :, :] = grad[0, at, side - n :, :] + below[at]


def rows_kernel(grad, before, after, down1, up1):
    w = before.shape[0]
    tiles, side = grad.shape[1], grad.shape[2]
    n = down1.shape[1]
    for out, at in ((down1, slice(side - n, side)), (up1, slice(0, n))):
        out[:w] = grad[1, :w, at, :] + before[:, at, :]
        out[w : tiles - w] = grad[1, w : tiles - w, at, :]
        out[tiles - w :] = grad[1, tiles - w :, at, :] + after[:, at, :]


def second_kernel(step_size, *refs):
    count_ref, first_ref, pos_ref, tab_ref, probe_ref, sorted_ref = refs[:6]
    old, g1, above0, below0, before0, after0, before1, after1, above1, below1, plane, other = refs[6:18]
    grad, new_ref, new_probe, down_r, down_l, low_r, send_ref, keep_ref = refs[18:26]
    ext, win, pro, gprobe_ref = refs[26:]
    n, side, tiles = probe_ref.shape[1], ext.shape[2], ext.shape[1]
    tile, w = side - n, n // LANES
    t = tile // LANES
    step_probe(probe_ref, plane, other, new_probe, step_size)
    inside_col = jnp.where(lax.axis_index("col") < lax.axis_size("col") - 1, 0.1, 0.0)
    inside_row = jnp.where(lax.axis_index("row") < lax.axis_size("row") - 1, 1.0, 0.0)
    for p, (above, below, before, after) in enumerate(
        ((above0, below0, before0, after0), (above1, below1, before1, after1))
    ):
        for j in range(tiles):
            weight = 0.1 if j < t else inside_col
            for r0, r1, side_rows in ((0, n, above), (n, tile, None), (tile, side, below)):
                total = g1[p, j, r0:r1, :]
                if side_rows is not None:
                    total = total + side_rows[j]
                if j < w:
                    total = total + before[j, r0:r1, :]
                if j >= t:
                    total = total + after[j - t, r0:r1, :]
                scale = weight * inside_row if r0 == tile else weight
                ext[p, j, r0:r1, :] = old[p, j, r0:r1, :] - scale * total
    for p in range(2):
        for j in range(t):
            new_ref[p, :, j * LANES : (j + 1) * LANES] = ext[p, j, :tile, :]
    grad[...] = jnp.zeros_like(grad)
    gprobe_ref[...] = jnp.zeros_like(gprobe_ref)
    stop = count_ref[0, 0]
    start = jnp.minimum(first_ref[0, 0], stop)
    frame_loop(start, stop, pos_ref, tab_ref, new_probe, sorted_ref, ext, grad, gprobe_ref, win, pro)
    core, seat = row_bits()
    members = lax.axis_size("row") // 2
    seat_order(gprobe_ref, 1 - core, seat, members, send_ref)
    seat_order(gprobe_ref, core, seat, members, keep_ref)
    down_r[...] = grad[:, t:, tile:, :]
    down_l[...] = grad[:, :t, tile:, :]
    low_r[...] = grad[:, t:, n:tile, :]


def join_kernel(grad, above, out):
    t, n = grad.shape[1] - above.shape[1], above.shape[2]
    out[...] = grad[:, t:, :n, :] + above[...]


def f32(*shape):
    return jax.ShapeDtypeStruct(shape, jnp.float32)


def vmem_call(kernel, out_shape, operands, scalars=(), scratch=(), limit=16):
    smem = [pl.BlockSpec(memory_space=pltpu.SMEM)] * len(scalars)
    vmem = pl.BlockSpec(memory_space=pltpu.VMEM)
    return pl.pallas_call(
        kernel,
        in_specs=smem + [vmem] * len(operands),
        out_specs=jax.tree.map(lambda _: vmem, out_shape),
        out_shape=out_shape,
        scratch_shapes=list(scratch),
        compiler_params=pltpu.CompilerParams(vmem_limit_bytes=limit * 1024 * 1024),
    )(*scalars, *operands)


def swap(value, axis, mask):
    count = lax.axis_size(axis)
    return lax.ppermute(value, axis, [(source, source ^ mask) for source in range(count)])


def row_bits():
    row = lax.axis_index("row")
    return lax.bitwise_and(row, 1), lax.shift_right_logical(row, 1)


def deal_kernel(keep_ref, heard_ref, *outs):
    height = outs[0].shape[0]
    for j, out in enumerate(outs):
        rows = slice(j * height, (j + 1) * height)
        out[...] = keep_ref[rows, :] + heard_ref[rows, :]


def steps_of(cols):
    steps = []
    step = 1
    while step < cols:
        steps.append(step)
        step *= 4
    return steps


def sum_probe(send, keep):
    members = lax.axis_size("row") // 2
    cols = lax.axis_size("col")
    height, width = keep.shape[0] // members, keep.shape[1]
    heard = swap(send, "row", 1)
    dealt = vmem_call(deal_kernel, [f32(height, width)] * members, (keep, heard))
    total = dealt[0]
    for value in [swap(dealt[j], "row", 2 * j) for j in range(1, members)]:
        total = total + value
    for step in steps_of(cols):
        near, *rest = [swap(total, "col", m * step) for m in (1, 2, 3) if m * step < cols]
        total = total + near
        if rest:
            total = total + (rest[0] + rest[1])
    parts = [total] + [swap(total, "row", 2 * j) for j in range(1, members)]
    plane = jnp.concatenate(parts, axis=0)
    return plane, swap(plane, "row", 1)


def step_probe(old_ref, plane_ref, other_ref, new_ref, step_size):
    core, seat = row_bits()
    members = lax.axis_size("row") // 2
    height = plane_ref.shape[0] // members
    for j in range(members):
        rows = pl.ds(pl.multiple_of(lax.bitwise_xor(seat, j) * height, height), height)
        here = slice(j * height, (j + 1) * height)
        new_ref[core, rows, :] = old_ref[core, rows, :] - step_size * plane_ref[here, :]
        new_ref[1 - core, rows, :] = old_ref[1 - core, rows, :] - step_size * other_ref[here, :]


def finish_kernel(old_ref, grad, above, before_top, before_low, out_ref):
    n, w = above.shape[2], before_top.shape[1]
    tile = out_ref.shape[1]
    for p in range(2):
        for j in range(tile // LANES):
            here = slice(j * LANES, (j + 1) * LANES)
            top = grad[p, j, :n, :] + above[p, j]
            low = grad[p, j, n:tile, :]
            if j < w:
                top = top + before_top[p, j]
                low = low + before_low[p, j]
            out_ref[p, :n, here] = old_ref[p, :n, here] - 0.1 * top
            out_ref[p, n:, here] = old_ref[p, n:, here] - 0.1 * low


def per_device(object_field, illumination, measured, positions, frame_counts, first_count):
    n = illumination.shape[1]
    tile = object_field.shape[1]
    side = tile + n
    tiles, w, t = side // LANES, n // LANES, tile // LANES
    devices = lax.axis_size("row") * lax.axis_size("col")
    step_size = 0.5 / math.sqrt(devices * measured.shape[2])
    tables = half_tables(n)
    scalars = (frame_counts, first_count, positions[0, 0])
    o = object_field

    right_top = shift(o[:, :n, :n], "col", -1)
    right_low = shift(o[:, n:, :n], "col", -1)
    below = shift(o[:, :n, :], "row", -1)
    order = sorter(n)
    sorted_measured = vmem_call(
        sort_kernel, f32(*measured.shape[2:]), (order, order.T, measured[0, 0]), (frame_counts,)
    )
    right_top, sorted_measured = lax.optimization_barrier((right_top, sorted_measured))
    corner = shift(right_top, "row", -1)

    work = [pltpu.VMEM((2,) + illumination.shape, jnp.float32)] * 2 + [pltpu.VMEM(illumination.shape, jnp.float32)]
    whole, plane_shape = f32(2, tiles, side, LANES), f32(n, n)
    row_strip, col_strip = f32(tiles, n, LANES), f32(w, side, LANES)
    ext, grad, down0, up0, right1, left1, send, keep = vmem_call(
        first_kernel,
        [whole, whole, row_strip, row_strip, col_strip, col_strip, plane_shape, plane_shape],
        (tables, illumination, sorted_measured, o, right_top, right_low, below, corner),
        scalars,
        work,
        28,
    )
    before1 = shift(right1, "col", 1)
    after1 = shift(left1, "col", -1)
    above0 = shift(down0, "row", 1)
    below0 = shift(up0, "row", -1)
    right0, left0 = vmem_call(columns_kernel, [col_strip] * 2, (grad, above0, below0))
    before0 = shift(right0, "col", 1)
    after0 = shift(left0, "col", -1)
    down1, up1 = vmem_call(rows_kernel, [row_strip] * 2, (grad, before1, after1))
    above1 = shift(down1, "row", 1)
    below1 = shift(up1, "row", -1)
    plane, other = sum_probe(send, keep)

    grad, new_object, new_probe, down_r, down_l, low_r, send, keep = vmem_call(
        lambda *refs: second_kernel(step_size, *refs),
        [whole, f32(*o.shape), f32(*illumination.shape), f32(2, w, n, LANES), f32(2, t, n, LANES),
         f32(2, w, tile - n, LANES), plane_shape, plane_shape],
        (tables, illumination, sorted_measured, ext, grad, above0, below0, before0, after0,
         before1, after1, above1, below1, plane, other),
        scalars,
        [pltpu.VMEM(whole.shape, jnp.float32)] + work,
        28,
    )
    above_r = shift(down_r, "row", 1)
    before_low = shift(low_r, "col", 1)
    above_l = shift(down_l, "row", 1)
    joined = vmem_call(join_kernel, f32(*above_r.shape), (grad, above_r))
    before_top = shift(joined, "col", 1)
    new_object = vmem_call(finish_kernel, f32(*o.shape), (new_object, grad, above_l, before_top, before_low))
    plane, other = sum_probe(send, keep)
    new_probe = vmem_call(
        lambda *refs: step_probe(*refs, step_size), f32(*illumination.shape), (new_probe, plane, other)
    )
    return (new_object, new_probe)


def solution(mesh):
    in_specs = (
        P(None, "row", "col"),
        P(),
        P("row", "col", None, None, None),
        P("row", "col", None, None),
        P("row", "col"),
        P("row", "col"),
    )
    out_specs = (P(None, "row", "col"), P())
    return jax.shard_map(per_device, mesh=mesh, in_specs=in_specs, out_specs=out_specs, check_vma=False)
```
